32 devices in a mesh: seq: 8 (over z, y), batch: 4 (over x, core).
Axes of the slice: x: 2, y: 2, z: 4, core: 2. Of those that a mesh axis runs over, the one named last changes fastest.
Arguments:
- q_nope: bfloat16 [4, 64, 128, 128], P('batch', None, 'seq'), may hold values from -6 to 6
- q_rope: bfloat16 [4, 64, 128, 64], P('batch', None, 'seq'), may hold values from -8 to 8
- absorb_k: bfloat16 [128, 128, 512], P('seq'), may hold values from -0.5 to 0.5
- absorb_v: bfloat16 [128, 512, 128], P('seq'), may hold values from -0.25 to 0.25
- cache_latent: bfloat16 [4, 8192, 512], P('batch', 'seq'), may hold values from -6 to 6
- cache_rope: bfloat16 [4, 8192, 64], P('batch', 'seq'), may hold values from -8 to 8
- draft_latent: bfloat16 [4, 64, 512], P('batch'), may hold values from -6 to 6
- draft_rope: bfloat16 [4, 64, 64], P('batch'), may hold values from -6 to 6
- residual: bfloat16 [256, 7168], P('batch', 'seq'), may hold values from -1.2 to 1.2
- out_proj: bfloat16 [16384, 7168], P('seq'), may hold values from -0.046875 to 0.046875
- norm_gain: float32 [7168], replicated, may hold values from 0.5 to 1.5
- lm_head: bfloat16 [65536, 7168], P(('seq', 'batch')), may hold values from -2.4095235 to 2.4095235
- parent: int32 [4, 64], replicated, may hold values from 0 to 62, as said below
- draft_ids: int32 [4, 64], replicated, may hold values from 0 to 65535
- cache_len: int32 [4], P('batch'), may hold values from 2048 to 8192
- accept_len: int32 [4], P('batch'), may hold values from 1 to 64
Outputs:
- hidden_out: bfloat16 [256, 7168], P('batch', 'seq')
- target_logp: float32 [4, 64], P('batch')
- accepted_score: float32 [4], P('batch')
The draws below stay inside these ranges and needn't reach their ends.
Inputs may be any that keep to these rules, and one draw needn't show every extreme that they name: parent[b, 0] = 0, and 0 <= parent[b, i] < i for i >= 1.
All inputs are finite; a program needn't handle non-finite values.
Results may differ from the reference program's by a relative error of at most 0.0095.
Values may be sent and summed in bfloat16 or wider, within the bound.
No kernel may reach another device: no remote copies, remote signals or barrier semaphores. Data moves between devices by JAX's collectives and lax.ppermute only.
A program may use at most 256 MiB of HBM per device.

```python
import math
import jax
import jax.numpy as jnp
from jax import lax

H = 128
HN = 128
HR = 64
C = 512
D = 7168
VOCAB = 65536
DRAFT = 64
REQUESTS = 4
LENGTH = 8192
TOKENS = 256


def draw_q_rope(key, part):
    full_shape = (REQUESTS, DRAFT, H, HR)
    values = jnp.clip(jax.random.normal(jax.random.fold_in(key, 11), full_shape, jnp.float32), -6.0, 6.0)
    return values.astype(jnp.bfloat16)


def draw_cache_rope(key, part):
    full_shape = (REQUESTS, LENGTH, HR)
    values = jnp.clip(jax.random.normal(jax.random.fold_in(key, 13), full_shape, jnp.float32), -6.0, 6.0)
    return values.astype(jnp.bfloat16)


def draw_residual(key, part):
    columns = jnp.arange(D, dtype=jnp.float32) / (D - 1)
    column_scale = 0.05 * (1.0 + 2.0 * columns)
    values = jnp.clip(jax.random.normal(jax.random.fold_in(key, 17), (TOKENS, D), jnp.float32), -6.0, 6.0)
    return (values * column_scale).astype(jnp.bfloat16)


def draw_lm_head(key, part):
    entries = jnp.arange(VOCAB, dtype=jnp.float32) / (VOCAB - 1)
    row_scale = (jnp.exp(jnp.log(3.0) * entries) / jnp.sqrt(jnp.float32(D)))[:, None]
    values = jnp.clip(jax.random.normal(jax.random.fold_in(key, 19), (VOCAB, D), jnp.float32), -6.0, 6.0) * row_scale
    return values.astype(jnp.bfloat16)


def draw_parent(key, part):
    choices_drawn = jax.random.randint(jax.random.fold_in(key, 3), (REQUESTS, DRAFT), 0, 1 << 20, dtype=jnp.int32)
    indices = jnp.arange(DRAFT, dtype=jnp.int32)
    spread = jnp.maximum(jnp.minimum(indices, 4), 1)
    parents = jnp.where(indices[None, :] == 0, 0, indices[None, :] - 1 - choices_drawn % spread[None, :])
    return parents.astype(jnp.int32)


def plant(array, key, low, largest):
    longest = array.shape.index(max(array.shape))
    spots = []
    for shift in (0, 1):
        where = [jax.random.randint(jax.random.fold_in(key, axis), (), 0, length) for axis, length in enumerate(array.shape)]
        where[longest] = (where[longest] + shift) % array.shape[longest]
        spots.append(tuple(where))
    return array.at[spots[0]].set(low).at[spots[1]].set(largest)


def block_scale(rng, dims, pieces, smallest, largest):
    loudness, own = 1.0, jax.random.fold_in(rng, 6)
    for dim, shards_of in pieces:
        steps = jnp.exp(jax.random.uniform(jax.random.fold_in(own, dim), (shards_of,), jnp.float32, smallest / len(pieces), largest / len(pieces)))
        loudness = loudness * jnp.repeat(steps, dims[dim] // shards_of).reshape([-1 if axis == dim else 1 for axis in range(len(dims))])
    return loudness


def normal_values(stream_key, dims, width, limit, cuts=(), held_as=jnp.bfloat16):
    level = block_scale(stream_key, dims, cuts, -0.22, 0.18) if cuts else 1.0
    values = jax.random.normal(stream_key, dims, jnp.float32) * width * level
    return jnp.minimum(jnp.maximum(values, -limit), limit).astype(held_as)


def setup_inputs(seed: int = 0) -> dict:
    seeds = jax.random.split(jax.random.key(seed), 17)
    q_nope = normal_values(seeds[0], (REQUESTS, DRAFT, H, HN), 1.0, 6.0, ((0, 4), (2, 8)))
    q_rope = draw_q_rope(jax.random.fold_in(seeds[16], 71), 0)
    absorb_k = normal_values(seeds[2], (H, HN, C), HN ** -0.5, 0.5, ((0, 8),))
    absorb_v = normal_values(seeds[3], (H, C, HN), C ** -0.5, 0.25, ((0, 8),))
    cache_latent = normal_values(seeds[4], (REQUESTS, LENGTH, C), 1.0, 6.0, ((0, 4), (1, 8)))
    cache_rope = draw_cache_rope(jax.random.fold_in(seeds[16], 71), 0)
    draft_latent = normal_values(seeds[6], (REQUESTS, DRAFT, C), 1.0, 6.0, ((0, 4),))
    draft_rope = normal_values(seeds[7], (REQUESTS, DRAFT, HR), 1.0, 6.0, ((0, 4),))
    residual = draw_residual(jax.random.fold_in(seeds[16], 71), 0)
    out_proj = normal_values(seeds[9], (H * HN, D), (H * HN) ** -0.5, 0.046875, ((0, 8),))
    norm_gain = jnp.clip(1.0 + 0.1 * jax.random.normal(seeds[10], (D,), jnp.float32), 0.5, 1.5)
    lm_head = draw_lm_head(jax.random.fold_in(seeds[16], 71), 0)
    parent = draw_parent(jax.random.fold_in(seeds[16], 71), 0)
    draft_ids = plant(jax.random.randint(seeds[13], (REQUESTS, DRAFT), 0, VOCAB), jax.random.fold_in(seeds[13], 1), 0, VOCAB - 1).astype(jnp.int32)
    cache_len = plant(jax.random.randint(seeds[14], (REQUESTS,), LENGTH // 4, LENGTH + 1), jax.random.fold_in(seeds[14], 1), LENGTH // 4, LENGTH).astype(jnp.int32)
    accept_len = plant(jax.random.randint(seeds[15], (REQUESTS,), 1, DRAFT + 1), jax.random.fold_in(seeds[15], 1), 1, DRAFT).astype(jnp.int32)
    return dict(q_nope=q_nope, q_rope=q_rope, absorb_k=absorb_k, absorb_v=absorb_v, cache_latent=cache_latent, cache_rope=cache_rope, draft_latent=draft_latent, draft_rope=draft_rope, residual=residual, out_proj=out_proj, norm_gain=norm_gain, lm_head=lm_head, parent=parent, draft_ids=draft_ids, cache_len=cache_len, accept_len=accept_len)


masked_value = -1e+30
norm_epsilon = 1e-06
highest = lax.Precision.HIGHEST

def ancestry_of(parents):
    draft_count = parents.shape[1]
    indices = jnp.arange(draft_count, dtype=jnp.int32)
    parent_map = ((parents[:, :, None] == indices[None, None, :]) & (indices[None, :, None] > 0)).astype(jnp.float32)
    ancestry = jnp.broadcast_to(jnp.eye(draft_count, dtype=jnp.float32), parent_map.shape)
    for doubling in range(draft_count.bit_length() - 1):
        ancestry = ancestry + jnp.einsum('rij,rjk->rik', ancestry, parent_map, precision=highest)
        parent_map = jnp.einsum('rij,rjk->rik', parent_map, parent_map, precision=highest)
    return ancestry > 0.5

def rounded(values):
    return lax.optimization_barrier(values.astype(jnp.bfloat16)).astype(jnp.float32)

def reference(q_nope, q_rope, absorb_k, absorb_v, cache_latent, cache_rope, draft_latent, draft_rope, residual, out_proj, norm_gain, lm_head, parent, draft_ids, cache_len, accept_len):
    score_scale = 1.0 / math.sqrt(HN + HR)
    ancestry = ancestry_of(parent)
    head_block = min(H, 16)
    absorb_k32 = absorb_k.astype(jnp.float32)
    absorb_v32 = absorb_v.astype(jnp.float32)

    def one_request(inputs):
        nope_query, rope_query, latent_cache, rope_cache, latent_draft, rope_draft, length, ancestors = inputs
        query_latent = rounded(jnp.einsum('ihn,hnc->ihc', nope_query.astype(jnp.float32), absorb_k32, precision=highest))
        rope_all = rope_query.astype(jnp.float32)
        latent32 = latent_cache.astype(jnp.float32)
        rope32 = rope_cache.astype(jnp.float32)
        draft32 = latent_draft.astype(jnp.float32)
        draft_rope32 = rope_draft.astype(jnp.float32)
        in_cache = jnp.arange(LENGTH, dtype=jnp.int32) < length

        def per_block(block_index):
            first = (block_index * head_block).astype(jnp.int32)
            query_part = lax.dynamic_slice_in_dim(query_latent, first, head_block, 1)
            rope_part = lax.dynamic_slice_in_dim(rope_all, first, head_block, 1)
            cache_scores = jnp.einsum('ihc,tc->hit', query_part, latent32, precision=highest) + jnp.einsum('ihe,te->hit', rope_part, rope32, precision=highest)
            cache_scores = jnp.where(in_cache[None, None, :], cache_scores * score_scale, masked_value)
            tree_scores = jnp.einsum('ihc,jc->hij', query_part, draft32, precision=highest) + jnp.einsum('ihe,je->hij', rope_part, draft_rope32, precision=highest)
            tree_scores = jnp.where(ancestors[None, :, :], tree_scores * score_scale, masked_value)
            row_top = jnp.maximum(lax.optimization_barrier(jnp.max(cache_scores, axis=2)), lax.optimization_barrier(jnp.max(tree_scores, axis=2)))
            cache_weights = jnp.exp(cache_scores - row_top[:, :, None])
            tree_weights = jnp.exp(tree_scores - row_top[:, :, None])
            weight_total = lax.optimization_barrier(jnp.sum(cache_weights, axis=2)) + lax.optimization_barrier(jnp.sum(tree_weights, axis=2))
            latent_sum = jnp.einsum('hit,tc->hic', rounded(cache_weights), latent32, precision=highest) + jnp.einsum('hij,jc->hic', rounded(tree_weights), draft32, precision=highest)
            value_part = lax.dynamic_slice_in_dim(absorb_v32, first, head_block, 0)
            projected = jnp.einsum('hic,hcn->hin', latent_sum, value_part, precision=highest)
            return (projected / weight_total[:, :, None]).astype(jnp.bfloat16)
        blocks = lax.map(per_block, jnp.arange(H // head_block, dtype=jnp.int32))
        return jnp.transpose(blocks.reshape(H, DRAFT, HN), (1, 0, 2)).reshape(DRAFT, H * HN)
    head_rows = lax.map(one_request, (q_nope, q_rope, cache_latent, cache_rope, draft_latent, draft_rope, cache_len, ancestry))
    head_rows = head_rows.reshape(TOKENS, H * HN)
    stream = residual.astype(jnp.float32) + jnp.dot(head_rows, out_proj, preferred_element_type=jnp.float32)
    hidden_out = stream.astype(jnp.bfloat16)
    mean_square = lax.optimization_barrier(jnp.mean(stream * stream, axis=1, keepdims=True))
    normed = (stream * lax.rsqrt(mean_square + norm_epsilon) * norm_gain).astype(jnp.bfloat16)
    logits = jnp.dot(normed, lm_head.T, preferred_element_type=jnp.float32)
    row_top = lax.optimization_barrier(jnp.max(logits, axis=1))
    log_total = row_top + jnp.log(lax.optimization_barrier(jnp.sum(jnp.exp(logits - row_top[:, None]), axis=1)))
    parent_rows = (jnp.arange(REQUESTS, dtype=jnp.int32)[:, None] * DRAFT + parent).reshape(-1)
    chosen = logits[parent_rows, draft_ids.reshape(-1)]
    target_logp = (chosen - log_total[parent_rows]).reshape(REQUESTS, DRAFT)
    accepted_score = lax.optimization_barrier(jnp.sum(jnp.where(jnp.arange(DRAFT, dtype=jnp.int32)[None, :] < accept_len[:, None], target_logp, 0.0), axis=1))
    return (hidden_out, target_logp, accepted_score)
```

```python
import functools
import math

import jax
import jax.numpy as jnp
from jax import lax
from jax.experimental import pallas as pl
from jax.experimental.pallas import tpu as pltpu
from jax.sharding import PartitionSpec as P

masked_value = -1e30
norm_epsilon = 1e-06
highest = lax.Precision.HIGHEST
f32 = jnp.float32
bf16 = jnp.bfloat16
MIB = 1 << 20
ATTEND_MIB = 20
ROW_TILE = 256
NT = (((1,), (1,)), ((), ()))
TN = (((0,), (0,)), ((), ()))


def ancestry_of(parents):
    draft_count = parents.shape[1]
    indices = jnp.arange(draft_count, dtype=jnp.int32)
    parent_map = (
        (parents[:, :, None] == indices[None, None, :]) & (indices[None, :, None] > 0)
    ).astype(f32)
    ancestry = jnp.broadcast_to(jnp.eye(draft_count, dtype=f32), parent_map.shape)
    for doubling in range(draft_count.bit_length() - 1):
        ancestry = ancestry + jnp.einsum("rij,rjk->rik", ancestry, parent_map, precision=highest)
        parent_map = jnp.einsum("rij,rjk->rik", parent_map, parent_map, precision=highest)
    return ancestry


def full_spec(array):
    return pl.BlockSpec(array.shape, lambda *_: (0,) * array.ndim)


smem_spec = pl.BlockSpec(memory_space=pltpu.SMEM)
vmem_spec = pl.BlockSpec(memory_space=pltpu.VMEM)
any_spec = pl.BlockSpec(memory_space=pl.ANY)


def ring_slot(shift, size):
    seq = lax.axis_index("seq")
    place = jnp.where(seq % 2 == 0, seq // 2, size - 1 - seq // 2)
    spot = (place + shift + size) % size
    return jnp.where(spot < size // 2, 2 * spot, 2 * (size - 1 - spot) + 1)


def in_vmem(array):
    return pltpu.with_memory_space_constraint(array, pltpu.VMEM)


def in_hbm(array):
    return pltpu.with_memory_space_constraint(array, pltpu.HBM)


def pack_kernel(latent_ref, rope_ref, out_ref, *, unit):
    rows, width = latent_ref.shape
    folds = width // unit
    group = rope_ref.shape[0] // folds
    for u in range(rows // unit):
        base = u * (unit + group)
        out_ref[base : base + unit, :] = latent_ref[u * unit : (u + 1) * unit, :]
        for f in range(folds):
            out_ref[base + unit : base + unit + group, f * unit : (f + 1) * unit] = rope_ref[
                f * group : (f + 1) * group, u * unit : (u + 1) * unit
            ]


def pack(latent, rope, unit):
    rows, width = latent.shape
    return pl.pallas_call(
        functools.partial(pack_kernel, unit=unit),
        in_specs=[vmem_spec, vmem_spec],
        out_specs=vmem_spec,
        out_shape=jax.ShapeDtypeStruct((rows + rows * rope.shape[0] // width, width), bf16),
        compiler_params=pltpu.CompilerParams(vmem_limit_bytes=12 * MIB),
        name="pack",
    )(latent, rope)


def fetch_kernel(weight_ref, after_ref, out_ref, token_ref, sems, *, shifts, seq_size):
    pieces, _, columns = out_ref.shape
    copies = []
    for k in range(pieces):
        other = 1 - lax.axis_index("seq") % 2
        slot = 2 * k + other if shifts is None else ring_slot(shifts[k], seq_size)
        copies.append(
            pltpu.make_async_copy(
                weight_ref.at[:, pl.ds(pl.multiple_of(slot * columns, 128), columns)],
                out_ref.at[k],
                sems.at[k],
            )
        )
    for copy in copies:
        copy.start()
    token_ref[...] = jnp.zeros_like(token_ref)
    for copy in copies:
        copy.wait()


def fetch(weight, seq_size, after, shifts=None):
    depth, width = weight.shape
    pieces = seq_size // 2 if shifts is None else len(shifts)
    return pl.pallas_call(
        functools.partial(fetch_kernel, shifts=shifts, seq_size=seq_size),
        in_specs=[any_spec, any_spec],
        out_specs=(vmem_spec, vmem_spec),
        out_shape=(
            pltpu.VMEM((pieces, depth, width // seq_size), weight.dtype),
            jax.ShapeDtypeStruct((8, 128), f32),
        ),
        scratch_shapes=[pltpu.SemaphoreType.DMA((pieces,))],
        compiler_params=pltpu.CompilerParams(vmem_limit_bytes=2 * MIB),
        cost_estimate=pl.CostEstimate(
            flops=depth * width * 512 * pieces // seq_size,
            transcendentals=0,
            bytes_accessed=2 * depth * width * pieces // seq_size,
        ),
        name="fetch",
    )(in_hbm(weight), after)


def attend_kernel(
    *refs, counts, spots, unit, tree, last, first, scale, tile_heads, seq_size, cache_rows
):
    refs = list(refs)
    length_ref, query_ref, rope_ref = refs[:3]
    del refs[:3]
    block_refs = refs[: len(counts)]
    del refs[: len(counts)]
    if tree:
        draft_ref, draft_rope_ref, mask_ref = refs[:3]
        del refs[:3]
    if not first:
        top_in, total_in, sum_in = refs[:3]
        del refs[:3]
    if last:
        value_ref, out_ref = refs[:2]
        del refs[:2]
    else:
        top_out, total_out, sum_out = refs[:3]
        del refs[:3]
    width = query_ref.shape[1]
    rope_width = rope_ref.shape[1]
    folds = width // unit
    group = rope_width // folds

    query = query_ref[...]
    rope = rope_ref[...]
    scores = []
    values = []
    for k, count in enumerate(counts):
        shift, offset = spots[k]
        valid = length_ref[0] - ring_slot(shift, seq_size) * cache_rows - offset
        for piece in range(count):
            base = piece * (unit + group)
            keys = block_refs[k][base : base + unit, :]
            score = lax.dot_general(query, keys, NT, preferred_element_type=f32)
            key_rope = jnp.concatenate(
                [
                    block_refs[k][
                        base + unit : base + unit + group, f * unit : (f + 1) * unit
                    ]
                    for f in range(folds)
                ],
                axis=0,
            )
            score = score + jnp.dot(rope, key_rope, preferred_element_type=f32)
            column = lax.broadcasted_iota(jnp.int32, score.shape, 1) + piece * unit
            scores.append(jnp.where(column < valid, score * scale, masked_value))
            values.append(keys)
    if tree:
        drafts = draft_ref[...]
        score = lax.dot_general(query, drafts, NT, preferred_element_type=f32)
        score = score + lax.dot_general(rope, draft_rope_ref[...], NT, preferred_element_type=f32)
        mask = jnp.concatenate([mask_ref[...]] * tile_heads, axis=0)
        scores.append(jnp.where(mask > 0.5, score * scale, masked_value))
        values.append(drafts)
    tops = [jnp.max(score, axis=1, keepdims=True) for score in scores]
    top = functools.reduce(jnp.maximum, tops)
    if not first:
        old_top = top_in[:, 0:1]
        top = jnp.maximum(top, old_top)
    total = None
    summed = None
    for score, keys in zip(scores, values):
        weight = jnp.exp2(score - top)
        part = jnp.sum(weight, axis=1, keepdims=True)
        product = jnp.dot(weight.astype(bf16), keys, preferred_element_type=f32)
        total = part if total is None else total + part
        summed = product if summed is None else summed + product
    if not first:
        shrink = jnp.exp2(old_top - top)
        total = total + total_in[:, 0:1] * shrink
        summed = summed + sum_in[...] * shrink
    if last:
        rows = query_ref.shape[0] // tile_heads
        columns = value_ref.shape[2]
        for head in range(tile_heads):
            span = slice(head * rows, (head + 1) * rows)
            projected = jnp.dot(
                summed[span].astype(bf16), value_ref[head], preferred_element_type=f32
            )
            out_ref[:, head * columns : (head + 1) * columns] = (projected / total[span]).astype(bf16)
    else:
        top_out[...] = jnp.broadcast_to(top, top_out.shape)
        total_out[...] = jnp.broadcast_to(total, total_out.shape)
        sum_out[...] = summed


def attend(
    length, query, rope, blocks, spots, *, unit, draft_count, scale, seq_size, cache_rows,
    state=None, tree=None, absorb_v=None,
):
    rows, width = query.shape
    rope_width = rope.shape[1]
    tile_heads = max(1, ROW_TILE // draft_count)
    while (rows // draft_count) % tile_heads:
        tile_heads -= 1
    tile = tile_heads * draft_count
    packed_unit = unit + unit * rope_width // width
    counts = tuple(b.shape[0] // packed_unit for b in blocks)
    row_spec = lambda columns: pl.BlockSpec((tile, columns), lambda i: (i, 0))
    blocks = [in_vmem(b) for b in blocks]
    operands = [length, query, rope, *blocks]
    in_specs = [smem_spec, row_spec(width), row_spec(rope_width)] + [full_spec(b) for b in blocks]
    if tree is not None:
        operands += list(tree)
        in_specs += [full_spec(t) for t in tree]
    aliases = {}
    if state is not None:
        if absorb_v is None:
            aliases = {len(operands) + k: k for k in range(3)}
        operands += list(state)
        in_specs += [row_spec(128), row_spec(128), row_spec(width)]
    if absorb_v is not None:
        columns = absorb_v.shape[2]
        operands.append(absorb_v)
        in_specs.append(pl.BlockSpec((tile_heads, width, columns), lambda i: (i, 0, 0)))
        out_shape = jax.ShapeDtypeStruct((draft_count, rows // draft_count * columns), bf16)
        out_specs = pl.BlockSpec((draft_count, tile_heads * columns), lambda i: (0, i))
    else:
        out_shape = (
            jax.ShapeDtypeStruct((rows, 128), f32),
            jax.ShapeDtypeStruct((rows, 128), f32),
            jax.ShapeDtypeStruct((rows, width), f32),
        )
        out_specs = (row_spec(128), row_spec(128), row_spec(width))
    keys = sum(counts) * unit
    return pl.pallas_call(
        functools.partial(
            attend_kernel,
            counts=counts,
            spots=tuple(spots),
            unit=unit,
            tree=tree is not None,
            last=absorb_v is not None,
            first=state is None,
            scale=scale,
            tile_heads=tile_heads,
            seq_size=seq_size,
            cache_rows=cache_rows,
        ),
        grid=(rows // tile,),
        in_specs=in_specs,
        out_specs=out_specs,
        out_shape=out_shape,
        input_output_aliases=aliases,
        compiler_params=pltpu.CompilerParams(vmem_limit_bytes=ATTEND_MIB * MIB),
        cost_estimate=pl.CostEstimate(
            flops=2 * rows * keys * (2 * width + rope_width),
            transcendentals=rows * keys,
            bytes_accessed=2 * keys * (width + rope_width) + 8 * rows * width,
        ),
        name="attend",
    )(*operands)


def project_kernel(rows_ref, weight_ref, out_ref, *, start):
    pieces, _, columns = out_ref.shape
    rows = rows_ref[...]
    for j in range(pieces):
        out_ref[j] = jnp.dot(
            rows, weight_ref[j, :, start : start + columns], preferred_element_type=f32
        ).astype(bf16)


def project(rows, weight, start, columns):
    count, depth = rows.shape
    pieces = weight.shape[0]
    return pl.pallas_call(
        functools.partial(project_kernel, start=start),
        in_specs=[vmem_spec, vmem_spec],
        out_specs=vmem_spec,
        out_shape=jax.ShapeDtypeStruct((pieces, count, columns), bf16),
        compiler_params=pltpu.CompilerParams(vmem_limit_bytes=8 * MIB),
        cost_estimate=pl.CostEstimate(
            flops=2 * count * depth * pieces * columns,
            transcendentals=0,
            bytes_accessed=2 * depth * pieces * columns,
        ),
        name="project",
    )(rows, in_vmem(weight))


def stream_kernel(rows_ref, weight_ref, after_ref, out_ref, buffer, sems):
    pieces, _, columns = out_ref.shape
    own = lax.axis_index("seq") % 2
    copies = []
    for k in range(pieces):
        first = pl.multiple_of((2 * k + own) * columns, 128)
        copies.append(
            pltpu.make_async_copy(
                weight_ref.at[:, pl.ds(first, columns)], buffer.at[k], sems.at[k]
            )
        )
    for copy in copies:
        copy.start()
    rows = rows_ref[...]
    for k in range(pieces):
        copies[k].wait()
        out_ref[k] = jnp.dot(rows, buffer[k], preferred_element_type=f32)


def project_near(rows, weight, seq_size, after):
    count, depth = rows.shape
    pieces = seq_size // 2
    columns = weight.shape[1] // seq_size
    return pl.pallas_call(
        stream_kernel,
        in_specs=[vmem_spec, any_spec, any_spec],
        out_specs=vmem_spec,
        out_shape=jax.ShapeDtypeStruct((pieces, count, columns), f32),
        scratch_shapes=[
            pltpu.VMEM((pieces, depth, columns), bf16),
            pltpu.SemaphoreType.DMA((pieces,)),
        ],
        compiler_params=pltpu.CompilerParams(vmem_limit_bytes=32 * MIB),
        cost_estimate=pl.CostEstimate(
            flops=2 * count * depth * pieces * columns,
            transcendentals=0,
            bytes_accessed=2 * depth * pieces * columns,
        ),
        name="project_near",
    )(rows, in_hbm(weight), after)


def fold_kernel(near_ref, far_ref, own_ref, *send_refs, start):
    pieces, _, columns = far_ref.shape
    here = lax.axis_index("seq") // 2
    for k in range(pieces):
        slot = (here + k) % pieces
        value = near_ref[slot, :, start : start + columns] + far_ref[slot].astype(f32)
        if k == 0:
            own_ref[...] = value
        else:
            send_refs[k - 1][...] = value.astype(bf16)


def fold(near, far, start):
    pieces, count, columns = far.shape
    return pl.pallas_call(
        functools.partial(fold_kernel, start=start),
        in_specs=[vmem_spec, vmem_spec],
        out_specs=(vmem_spec,) * pieces,
        out_shape=(jax.ShapeDtypeStruct((count, columns), f32),)
        + (jax.ShapeDtypeStruct((count, columns), bf16),) * (pieces - 1),
        compiler_params=pltpu.CompilerParams(vmem_limit_bytes=8 * MIB),
        name="fold",
    )(near, far)


def total_kernel(residual_ref, *refs):
    pieces = len(refs) // 2
    start = 0
    for group in (refs[:pieces], refs[pieces:-1]):
        if not group:
            continue
        columns = group[0].shape[1]
        value = residual_ref[:, start : start + columns].astype(f32) + group[0][...]
        for ref in group[1:]:
            value = value + ref[...].astype(f32)
        refs[-1][:, start : start + columns] = value.astype(bf16)
        start += columns


def total(residual, parts):
    operands = [residual, *parts]
    return pl.pallas_call(
        total_kernel,
        in_specs=[vmem_spec] * len(operands),
        out_specs=vmem_spec,
        out_shape=jax.ShapeDtypeStruct(residual.shape, bf16),
        compiler_params=pltpu.CompilerParams(vmem_limit_bytes=8 * MIB),
        name="total",
    )(*operands)


def vocab_kernel(*refs, shifts, following, first, last, halves, width_all, vocab_tile, seq_size, batch_size, drafts):
    refs = list(refs)
    blocks = len(shifts)
    row_refs = refs[: blocks * halves]
    del refs[: blocks * halves]
    gain_ref, weight_ref = refs[:2]
    del refs[:2]
    if not first:
        square_in, logit_in = refs[:2]
        del refs[:2]
    copies = []
    if last:
        ids_ref, parents_ref, out_ref, scaled_ref = refs
    else:
        source_ref, square_out, logit_out, next_ref, scaled_ref, sems = refs
    _, vocab, columns = weight_ref.shape
    tiles = vocab // vocab_tile
    first_of = lambda shift: pl.multiple_of(ring_slot(shift, seq_size) * columns, 128)
    firsts = [first_of(shift) for shift in shifts]
    for k, shift in enumerate(following):
        copies.append(
            pltpu.make_async_copy(
                source_ref.at[:, pl.ds(first_of(shift), columns)], next_ref.at[k], sems.at[k]
            )
        )
    for copy in copies:
        copy.start()
    square = None if first else square_in[...]
    for b in range(blocks):
        start = 0
        squares = []
        for part in range(halves):
            stream = row_refs[b * halves + part][...].astype(f32)
            rows = stream.shape[0]
            scaled_ref[b, start : start + rows, :] = (
                stream * gain_ref[:, pl.ds(firsts[b], columns)][0:1, :]
            ).astype(bf16)
            start += rows
            squared = stream * stream
            squares.append(
                sum(squared[:, k * 128 : (k + 1) * 128] for k in range(squared.shape[1] // 128))
            )
        squares = jnp.concatenate(squares, axis=0)
        square = squares if square is None else square + squares
    tokens = scaled_ref.shape[1]
    if last:
        mean = jnp.sum(jnp.transpose(square), axis=0, keepdims=True) / width_all
        shrink = lax.rsqrt(mean + norm_epsilon)
        vocab_first = (
            lax.axis_index("seq") * batch_size + lax.axis_index("batch")
        ) * vocab
        row = lax.broadcasted_iota(jnp.int32, (tokens, tokens), 0)
        choice = jnp.where(row == parents_ref[0:1, :], 1.0, 0.0).astype(bf16)
    else:
        square_out[...] = square
    tops, totals, picks = [], [], []
    for t in range(tiles):
        span = slice(t * vocab_tile, (t + 1) * vocab_tile)
        logits = None if first else logit_in[span, :]
        for b in range(blocks):
            product = lax.dot_general(
                weight_ref[b, span, :], scaled_ref[b], NT, preferred_element_type=f32
            )
            logits = product if logits is None else logits + product
        if not last:
            logit_out[span, :] = logits
            continue
        logits = logits * shrink
        top = jnp.max(logits, axis=0, keepdims=True)
        tops.append(top)
        totals.append(jnp.sum(jnp.exp(logits - top), axis=0, keepdims=True))
        column = lax.broadcasted_iota(jnp.int32, logits.shape, 0) + (vocab_first + t * vocab_tile)
        rest = logits
        source = None
        for _ in range(3):
            piece = rest.astype(bf16)
            rest = rest - piece.astype(f32)
            product = jnp.dot(piece, choice, preferred_element_type=f32)
            source = product if source is None else source + product
        picks.append(
            jnp.sum(jnp.where(column == ids_ref[0:1, :], source, 0.0), axis=0, keepdims=True)
        )
    for copy in copies:
        copy.wait()
    if not last:
        return
    best = functools.reduce(jnp.maximum, tops)
    mass = sum(total * jnp.exp(top - best) for top, total in zip(tops, totals))
    picked = sum(picks)
    pairs = batch_size // 2
    own = lax.axis_index("batch")
    pad = jnp.zeros((1, 128 - drafts), f32)
    for dc in range(2):
        for dx in range(pairs):
            g = (dc * pairs + dx) * drafts
            batch = ((own // 2 + dx) % pairs) * 2 + (own + dc) % 2
            line = jnp.concatenate(
                [x for v in (best, mass, picked) for x in (v[:, g : g + drafts], pad)], axis=1
            )
            for s in range(seq_size):
                out_ref[s * batch_size + batch] = line


def vocab_step(rows, shifts, table, gain, weight, sizes, drafts, state=None, final=None, following=()):
    blocks = len(rows)
    halves = len(rows[0])
    vocab, width_all = weight.shape
    columns = rows[0][0].shape[1]
    tokens = sum(r.shape[0] for r in rows[0])
    seq_size, batch_size = sizes
    operands = [r for parts in rows for r in parts] + [gain, in_vmem(table)]
    aliases = {}
    if state is not None:
        if final is None:
            aliases = {len(operands) + k: k for k in range(2)}
        operands += list(state)
    in_specs = [vmem_spec] * len(operands)
    scratch = [pltpu.VMEM((blocks, tokens, columns), bf16)]
    if final is not None:
        operands += list(final)
        in_specs += [vmem_spec] * 2
        out_shape = jax.ShapeDtypeStruct((seq_size * batch_size, 1, 384), f32)
        out_specs = vmem_spec
    else:
        operands.append(in_hbm(weight))
        in_specs.append(any_spec)
        out_shape = (
            jax.ShapeDtypeStruct((tokens, 128), f32),
            jax.ShapeDtypeStruct((vocab, tokens), f32),
            pltpu.VMEM((len(following), vocab, columns), bf16),
        )
        out_specs = (vmem_spec,) * 3
        scratch.append(pltpu.SemaphoreType.DMA((len(following),)))
    return pl.pallas_call(
        functools.partial(
            vocab_kernel,
            shifts=tuple(shifts),
            following=tuple(following),
            first=state is None,
            last=final is not None,
            halves=halves,
            width_all=width_all,
            vocab_tile=min(512, vocab),
            seq_size=seq_size,
            batch_size=batch_size,
            drafts=drafts,
        ),
        in_specs=in_specs,
        out_specs=out_specs,
        out_shape=out_shape,
        scratch_shapes=scratch,
        input_output_aliases=aliases,
        compiler_params=pltpu.CompilerParams(vmem_limit_bytes=12 * MIB),
        cost_estimate=pl.CostEstimate(
            flops=2 * tokens * vocab * columns * blocks,
            transcendentals=0,
            bytes_accessed=2 * vocab * columns * blocks + 8 * vocab * tokens,
        ),
        name="vocab",
    )(*operands)


def finish_kernel(accept_ref, stats_ref, parent_ref, target_ref, accepted_ref):
    drafts = target_ref.shape[1]
    stats = stats_ref[:, 0, :]
    tops, totals, picks = (stats[:, k * 128 : (k + 1) * 128] for k in range(3))
    best = jnp.max(tops, axis=0, keepdims=True)
    mass = jnp.sum(totals * jnp.exp(tops - best), axis=0, keepdims=True)
    chosen = jnp.sum(picks, axis=0, keepdims=True)
    log_total = best + jnp.log(mass)
    column = jnp.transpose(jnp.broadcast_to(log_total, (128, 128)))[:drafts, :drafts]
    parents = parent_ref[pl.ds(lax.axis_index("batch"), 1), :]
    row = lax.broadcasted_iota(jnp.int32, (drafts, drafts), 0)
    parent_total = jnp.sum(jnp.where(row == parents, column, 0.0), axis=0, keepdims=True)
    target = chosen[:, :drafts] - parent_total
    target_ref[...] = target
    index = lax.broadcasted_iota(jnp.int32, target.shape, 1)
    accepted_ref[...] = jnp.sum(
        jnp.where(index < accept_ref[0], target, 0.0), axis=1, keepdims=True
    )


def finish(stats, parent, accept_len, drafts):
    target, accepted = pl.pallas_call(
        finish_kernel,
        in_specs=[smem_spec, vmem_spec, vmem_spec],
        out_specs=(vmem_spec, vmem_spec),
        out_shape=(jax.ShapeDtypeStruct((1, drafts), f32), jax.ShapeDtypeStruct((1, 1), f32)),
        compiler_params=pltpu.CompilerParams(vmem_limit_bytes=4 * MIB),
        name="finish",
    )(accept_len, stats, parent)
    return target, accepted.reshape(1)


def plain_tail(head_rows, residual, out_proj, norm_gain, lm_head, parent, draft_ids, accept_len):
    draft_count = head_rows.shape[0]
    batch_index = lax.axis_index("batch")
    branch_term = jnp.dot(head_rows, out_proj, preferred_element_type=f32)
    width_local = residual.shape[1]
    feature_first = lax.axis_index("seq") * width_local
    stream_mine = residual.astype(f32) + lax.psum_scatter(
        branch_term, "seq", scatter_dimension=1, tiled=True
    )
    square = lax.psum(jnp.sum(stream_mine * stream_mine, axis=1), "seq")
    width_all = width_local * lax.axis_size("seq")
    gain_mine = lax.dynamic_slice_in_dim(norm_gain, feature_first, width_local, 0)
    normed_mine = (
        stream_mine * lax.rsqrt(square / width_all + norm_epsilon)[:, None] * gain_mine
    ).astype(bf16)
    normed = lax.all_gather(normed_mine, "seq", axis=1, tiled=True)
    hidden_out = stream_mine.astype(bf16)
    vocab_rows = lm_head.shape[0]
    vocab_first = lax.axis_index(("seq", "batch")) * vocab_rows
    logits = jnp.einsum(
        "rd,vd->rv",
        lax.all_gather(normed, "batch", axis=0, tiled=True),
        lm_head,
        preferred_element_type=f32,
    )
    request_total = parent.shape[0]
    parent_rows = (
        jnp.arange(request_total, dtype=jnp.int32)[:, None] * draft_count + parent
    ).reshape(-1)
    source = logits[parent_rows]
    column = jnp.arange(vocab_rows, dtype=jnp.int32) + vocab_first
    picked = jnp.sum(
        jnp.where(column[None, :] == draft_ids.reshape(-1)[:, None], source, 0.0), axis=1
    )
    best = lax.pmax(jnp.max(logits, axis=1), ("seq", "batch"))
    exp_mass, chosen = lax.psum(
        (jnp.sum(jnp.exp(logits - best[:, None]), axis=1), picked), ("seq", "batch")
    )
    log_total = best + jnp.log(exp_mass)
    target_all = (chosen - log_total[parent_rows]).reshape(request_total, draft_count)
    target_logp = lax.dynamic_slice_in_dim(target_all, batch_index, 1, 0)
    indices = jnp.arange(draft_count, dtype=jnp.int32)
    accepted_score = jnp.sum(
        jnp.where(indices[None, :] < accept_len[:, None], target_logp, 0.0), axis=1
    )
    return (hidden_out, target_logp, accepted_score)


def body(
    q_nope,
    q_rope,
    absorb_k,
    absorb_v,
    cache_latent,
    cache_rope,
    draft_latent,
    draft_rope,
    residual,
    out_proj,
    norm_gain,
    lm_head,
    parent,
    draft_ids,
    cache_len,
    accept_len,
    *,
    seq_size,
    batch_size,
):
    requests, draft_count, local_heads, nope_width = q_nope.shape
    assert requests == 1 and seq_size % 2 == 0 and batch_size % 2 == 0
    cache_rows, width = cache_latent.shape[1:]
    rope_width = q_rope.shape[3]
    scale = math.log2(math.e) / math.sqrt(nope_width + rope_width)
    batch_index = lax.axis_index("batch")

    order = [*range(0, seq_size, 2), *reversed(range(1, seq_size, 2))]
    forward = [(order[i], order[(i + 1) % seq_size]) for i in range(seq_size)]
    backward = [(b, a) for a, b in forward]
    move = lambda array, ring: lax.ppermute(array, "seq", ring)

    units = 4
    unit = cache_rows // units
    size = unit + unit * rope_width // width
    block = pack(cache_latent[0], jnp.swapaxes(cache_rope[0], 0, 1), unit)
    far = seq_size // 2
    left = move(block, forward)
    right = move(block, backward)

    query = jnp.einsum(
        "ihn,hnc->hic", q_nope[0], absorb_k, preferred_element_type=f32
    ).astype(bf16).reshape(local_heads * draft_count, width)
    rope = jnp.transpose(q_rope[0], (1, 0, 2)).reshape(local_heads * draft_count, rope_width)
    own_parents = lax.dynamic_slice_in_dim(parent, batch_index * requests, requests, 0)
    mask = ancestry_of(own_parents)[0]

    pairs = batch_size // 2
    own_pair, own_core = batch_index // 2, batch_index % 2
    group_batch = jnp.stack(
        [
            ((own_pair + dx) % pairs) * 2 + (own_core + dc) % 2
            for dc in range(2)
            for dx in range(pairs)
        ]
    )
    tokens = batch_size * draft_count
    id_row = draft_ids[group_batch].reshape(1, tokens)
    starts = jnp.arange(batch_size, dtype=jnp.int32)[:, None] * draft_count
    parent_row = (parent[group_batch] + starts).reshape(1, tokens)

    gain = jnp.broadcast_to(norm_gain[None, :], (8, norm_gain.shape[0]))
    run = functools.partial(
        attend,
        cache_len,
        query,
        rope,
        unit=unit,
        draft_count=draft_count,
        scale=scale,
        seq_size=seq_size,
        cache_rows=cache_rows,
    )
    state = run([block], [(0, 0)], tree=(draft_latent[0], draft_rope[0], mask))
    for k in range(1, far):
        left, right, state, id_row, parent_row, gain = lax.optimization_barrier(
            (left, right, state, id_row, parent_row, gain)
        )
        if k == 1:
            weight, token = fetch(out_proj, seq_size, left)
        else:
            left, right, token = lax.optimization_barrier((left, right, token))
        arrived = (left, right)
        if k < far - 1:
            left, right = move(left, forward), move(right, backward)
        else:
            low, high = [], []
            for q in range(2):
                low.append(move(left[q * size : (q + 1) * size], forward))
                high.append(move(right[(q + 2) * size : (q + 3) * size], backward))
        state = run(arrived, [(-k, 0), (k, 0)], state=state)
    state = run([low[0], high[0]], [(far, 0), (far, 2 * unit)], state=state)
    head_rows = run(
        [low[1], high[1]], [(far, unit), (far, 3 * unit)], state=state, absorb_v=absorb_v
    )

    columns = residual.shape[1]
    if columns % 128:
        return plain_tail(
            head_rows, residual, out_proj, norm_gain, lm_head, parent, draft_ids, accept_len
        )
    swap = [(s, s ^ 1) for s in range(seq_size)]
    split = (columns // 128 + 1) // 2 * 128
    spans = [(0, split), (split, columns - split)]
    sent = [project(head_rows, weight, *span) for span in spans]
    near = project_near(head_rows, out_proj, seq_size, sent[-1])
    sent = [lax.ppermute(x, "seq", swap) for x in sent]
    parts = []
    for (start, _), share in zip(spans, sent):
        own, *sends = fold(near, share, start)
        parts.append(own)
        for k, send in enumerate(sends):
            perm = [(s, (s + 2 * (k + 1)) % seq_size) for s in range(seq_size)]
            parts.append(lax.ppermute(send, "seq", perm))
    hidden_out = total(residual, parts)

    rows = [hidden_out]
    for k in range(1, pairs):
        perm = [(((x + k) % pairs) * 2 + c, x * 2 + c) for x in range(pairs) for c in range(2)]
        rows.append(lax.ppermute(hidden_out, "batch", perm))
    rows = jnp.concatenate(rows, axis=0)
    partner = [(b, b ^ 1) for b in range(batch_size)]
    twin = lambda r: (r, lax.ppermute(r, "batch", partner))
    step = functools.partial(
        vocab_step,
        gain=gain,
        weight=lm_head,
        sizes=(seq_size, batch_size),
        drafts=draft_count,
    )
    left = right = rows
    table, _ = fetch(lm_head, seq_size, hidden_out, shifts=(0,))
    arrived, shifts = [twin(rows)], (0,)
    state = None
    for k in range(1, far):
        left = lax.ppermute(left, "seq", forward)
        right = lax.ppermute(right, "seq", backward)
        *state, table = step(arrived, shifts, table, state=state, following=(-k, k))
        arrived, shifts = [twin(left), twin(right)], (-k, k)
    cut = rows.shape[0] // 2
    low = lax.ppermute(left[:cut], "seq", forward)
    high = lax.ppermute(right[cut:], "seq", backward)
    *state, table = step(arrived, shifts, table, state=state, following=(far,))
    ends = twin(jnp.concatenate([low, high], axis=0))
    stats = step([ends], (far,), table, state=state, final=(id_row, parent_row))
    stats = lax.all_to_all(stats, ("seq", "batch"), 0, 0, tiled=True)
    target_logp, accepted_score = finish(stats, parent, accept_len, draft_count)
    return (hidden_out, target_logp, accepted_score)


def solution(mesh):
    in_specs = (
        P("batch", None, "seq", None),
        P("batch", None, "seq", None),
        P("seq", None, None),
        P("seq", None, None),
        P("batch", "seq", None),
        P("batch", "seq", None),
        P("batch", None, None),
        P("batch", None, None),
        P("batch", "seq"),
        P("seq", None),
        P(),
        P(("seq", "batch"), None),
        P(),
        P(),
        P("batch"),
        P("batch"),
    )
    out_specs = (P("batch", "seq"), P("batch", None), P("batch"))
    sized = functools.partial(body, seq_size=mesh.shape["seq"], batch_size=mesh.shape["batch"])
    return jax.shard_map(sized, mesh=mesh, in_specs=in_specs, out_specs=out_specs, check_vma=False)
```

```python
import functools
import math

import jax
import jax.numpy as jnp
from jax import lax
from jax.experimental import pallas as pl
from jax.experimental.pallas import tpu as pltpu
from jax.sharding import PartitionSpec as P

masked_value = -1e30
norm_epsilon = 1e-06
highest = lax.Precision.HIGHEST
f32 = jnp.float32
bf16 = jnp.bfloat16
MIB = 1 << 20
ATTEND_MIB = 16
ROW_TILE = 256
NT = (((1,), (1,)), ((), ()))
TN = (((0,), (0,)), ((), ()))


def ancestry_of(parents):
    draft_count = parents.shape[1]
    indices = jnp.arange(draft_count, dtype=jnp.int32)
    parent_map = (
        (parents[:, :, None] == indices[None, None, :]) & (indices[None, :, None] > 0)
    ).astype(f32)
    ancestry = jnp.broadcast_to(jnp.eye(draft_count, dtype=f32), parent_map.shape)
    for doubling in range(draft_count.bit_length() - 1):
        ancestry = ancestry + jnp.einsum("rij,rjk->rik", ancestry, parent_map, precision=highest)
        parent_map = jnp.einsum("rij,rjk->rik", parent_map, parent_map, precision=highest)
    return ancestry


def full_spec(array):
    return pl.BlockSpec(array.shape, lambda *_: (0,) * array.ndim)


smem_spec = pl.BlockSpec(memory_space=pltpu.SMEM)
vmem_spec = pl.BlockSpec(memory_space=pltpu.VMEM)
any_spec = pl.BlockSpec(memory_space=pl.ANY)


def ring_slot(shift, size):
    seq = lax.axis_index("seq")
    place = jnp.where(seq % 2 == 0, seq // 2, size - 1 - seq // 2)
    spot = (place + shift + size) % size
    return jnp.where(spot < size // 2, 2 * spot, 2 * (size - 1 - spot) + 1)


def in_vmem(array):
    return pltpu.with_memory_space_constraint(array, pltpu.VMEM)


def in_hbm(array):
    return pltpu.with_memory_space_constraint(array, pltpu.HBM)


def pack_kernel(latent_ref, rope_ref, *out_refs, unit):
    rows, width = latent_ref.shape
    folds = width // unit
    group = rope_ref.shape[0] // folds
    units = rows // unit
    for u in range(units):
        out_ref = out_refs[2 * u // units]
        base = u % (units // 2) * (unit + group)
        out_ref[base : base + unit, :] = latent_ref[u * unit : (u + 1) * unit, :]
        for f in range(folds):
            out_ref[base + unit : base + unit + group, f * unit : (f + 1) * unit] = rope_ref[
                f * group : (f + 1) * group, u * unit : (u + 1) * unit
            ]


def pack(latent, rope, unit):
    rows, width = latent.shape
    half = jax.ShapeDtypeStruct(((rows + rows * rope.shape[0] // width) // 2, width), bf16)
    return pl.pallas_call(
        functools.partial(pack_kernel, unit=unit),
        in_specs=[vmem_spec, vmem_spec],
        out_specs=(vmem_spec, vmem_spec),
        out_shape=(half, half),
        compiler_params=pltpu.CompilerParams(vmem_limit_bytes=12 * MIB),
        name="pack",
    )(latent, rope)


def fetch_kernel(weight_ref, after_ref, out_ref, token_ref, sems, *, shifts, seq_size):
    pieces, _, columns = out_ref.shape
    copies = []
    for k in range(pieces):
        other = 1 - lax.axis_index("seq") % 2
        slot = 2 * k + other if shifts is None else ring_slot(shifts[k], seq_size)
        copies.append(
            pltpu.make_async_copy(
                weight_ref.at[:, pl.ds(pl.multiple_of(slot * columns, 128), columns)],
                out_ref.at[k],
                sems.at[k],
            )
        )
    for copy in copies:
        copy.start()
    token_ref[...] = jnp.zeros_like(token_ref)
    for copy in copies:
        copy.wait()


def fetch(weight, seq_size, after, shifts=None):
    depth, width = weight.shape
    pieces = seq_size // 2 if shifts is None else len(shifts)
    return pl.pallas_call(
        functools.partial(fetch_kernel, shifts=shifts, seq_size=seq_size),
        in_specs=[any_spec, any_spec],
        out_specs=(vmem_spec, vmem_spec),
        out_shape=(
            pltpu.VMEM((pieces, depth, width // seq_size), weight.dtype),
            jax.ShapeDtypeStruct((8, 128), f32),
        ),
        scratch_shapes=[pltpu.SemaphoreType.DMA((pieces,))],
        compiler_params=pltpu.CompilerParams(vmem_limit_bytes=2 * MIB),
        cost_estimate=pl.CostEstimate(
            flops=depth * width * 512 * pieces // seq_size,
            transcendentals=0,
            bytes_accessed=2 * depth * width * pieces // seq_size,
        ),
        name="fetch",
    )(in_hbm(weight), after)


def attend_kernel(
    *refs, counts, spots, unit, tree, last, first, scale, tile_heads, seq_size, cache_rows
):
    refs = list(refs)
    length_ref, query_ref, rope_ref, _ = refs[:4]
    del refs[:4]
    block_refs = refs[: len(counts)]
    del refs[: len(counts)]
    if tree:
        draft_ref, draft_rope_ref, mask_ref = refs[:3]
        del refs[:3]
    if not first:
        top_in, total_in, sum_in = refs[:3]
        del refs[:3]
    if last:
        value_ref, out_ref = refs[:2]
        del refs[:2]
    else:
        top_out, total_out, sum_out = refs[:3]
        del refs[:3]
    width = query_ref.shape[1]
    rope_width = rope_ref.shape[1]
    folds = width // unit
    group = rope_width // folds

    query = query_ref[...]
    rope = rope_ref[...]
    scores = []
    values = []
    for k, count in enumerate(counts):
        shift, offset = spots[k]
        valid = length_ref[0] - ring_slot(shift, seq_size) * cache_rows - offset
        for piece in range(count):
            base = piece * (unit + group)
            keys = block_refs[k][base : base + unit, :]
            score = lax.dot_general(query, keys, NT, preferred_element_type=f32)
            key_rope = jnp.concatenate(
                [
                    block_refs[k][
                        base + unit : base + unit + group, f * unit : (f + 1) * unit
                    ]
                    for f in range(folds)
                ],
                axis=0,
            )
            score = score + jnp.dot(rope, key_rope, preferred_element_type=f32)
            column = lax.broadcasted_iota(jnp.int32, score.shape, 1) + piece * unit
            scores.append(jnp.where(column < valid, score * scale, masked_value))
            values.append(keys)
    if tree:
        drafts = draft_ref[...]
        score = lax.dot_general(query, drafts, NT, preferred_element_type=f32)
        score = score + lax.dot_general(rope, draft_rope_ref[...], NT, preferred_element_type=f32)
        mask = jnp.concatenate([mask_ref[...]] * tile_heads, axis=0)
        scores.append(jnp.where(mask > 0.5, score * scale, masked_value))
        values.append(drafts)
    tops = [jnp.max(score, axis=1, keepdims=True) for score in scores]
    top = functools.reduce(jnp.maximum, tops)
    if not first:
        old_top = top_in[:, 0:1]
        top = jnp.maximum(top, old_top)
    total = None
    summed = None
    for score, keys in zip(scores, values):
        weight = jnp.exp2(score - top)
        part = jnp.sum(weight, axis=1, keepdims=True)
        product = jnp.dot(weight.astype(bf16), keys, preferred_element_type=f32)
        total = part if total is None else total + part
        summed = product if summed is None else summed + product
    if not first:
        shrink = jnp.exp2(old_top - top)
        total = total + total_in[:, 0:1] * shrink
        summed = summed + sum_in[...] * shrink
    if last:
        rows = query_ref.shape[0] // tile_heads
        columns = value_ref.shape[2]
        for head in range(tile_heads):
            span = slice(head * rows, (head + 1) * rows)
            projected = jnp.dot(
                summed[span].astype(bf16), value_ref[head], preferred_element_type=f32
            )
            out_ref[:, head * columns : (head + 1) * columns] = (projected / total[span]).astype(bf16)
    else:
        top_out[...] = jnp.broadcast_to(top, top_out.shape)
        total_out[...] = jnp.broadcast_to(total, total_out.shape)
        sum_out[...] = summed


def attend(
    length, query, rope, blocks, spots, *, unit, draft_count, scale, seq_size, cache_rows,
    state=None, tree=None, absorb_v=None, after=None,
):
    rows, width = query.shape
    rope_width = rope.shape[1]
    tile_heads = max(1, ROW_TILE // draft_count)
    while (rows // draft_count) % tile_heads:
        tile_heads -= 1
    tile = tile_heads * draft_count
    packed_unit = unit + unit * rope_width // width
    counts = tuple(b.shape[0] // packed_unit for b in blocks)
    row_spec = lambda columns: pl.BlockSpec((tile, columns), lambda i: (i, 0))
    blocks = [in_vmem(b) for b in blocks]
    operands = [length, query, rope, length if after is None else after, *blocks]
    in_specs = [smem_spec, row_spec(width), row_spec(rope_width), any_spec]
    in_specs += [full_spec(b) for b in blocks]
    if tree is not None:
        operands += list(tree)
        in_specs += [full_spec(t) for t in tree]
    aliases = {}
    if state is not None:
        if absorb_v is None:
            aliases = {len(operands) + k: k for k in range(3)}
        operands += list(state)
        in_specs += [row_spec(128), row_spec(128), row_spec(width)]
    if absorb_v is not None:
        columns = absorb_v.shape[2]
        operands.append(absorb_v)
        in_specs.append(pl.BlockSpec((tile_heads, width, columns), lambda i: (i, 0, 0)))
        out_shape = jax.ShapeDtypeStruct((draft_count, rows // draft_count * columns), bf16)
        out_specs = pl.BlockSpec((draft_count, tile_heads * columns), lambda i: (0, i))
    else:
        out_shape = (
            jax.ShapeDtypeStruct((rows, 128), f32),
            jax.ShapeDtypeStruct((rows, 128), f32),
            jax.ShapeDtypeStruct((rows, width), f32),
        )
        out_specs = (row_spec(128), row_spec(128), row_spec(width))
    keys = sum(counts) * unit
    return pl.pallas_call(
        functools.partial(
            attend_kernel,
            counts=counts,
            spots=tuple(spots),
            unit=unit,
            tree=tree is not None,
            last=absorb_v is not None,
            first=state is None,
            scale=scale,
            tile_heads=tile_heads,
            seq_size=seq_size,
            cache_rows=cache_rows,
        ),
        grid=(rows // tile,),
        in_specs=in_specs,
        out_specs=out_specs,
        out_shape=out_shape,
        input_output_aliases=aliases,
        compiler_params=pltpu.CompilerParams(vmem_limit_bytes=ATTEND_MIB * MIB),
        cost_estimate=pl.CostEstimate(
            flops=2 * rows * keys * (2 * width + rope_width),
            transcendentals=rows * keys,
            bytes_accessed=2 * keys * (width + rope_width) + 8 * rows * width,
        ),
        name="attend",
    )(*operands)


def project_kernel(rows_ref, weight_ref, out_ref, *, start):
    pieces, _, columns = out_ref.shape
    rows = rows_ref[...]
    for j in range(pieces):
        out_ref[j] = jnp.dot(
            rows, weight_ref[j, :, start : start + columns], preferred_element_type=f32
        ).astype(bf16)


def project(rows, weight, start, columns):
    count, depth = rows.shape
    pieces = weight.shape[0]
    return pl.pallas_call(
        functools.partial(project_kernel, start=start),
        in_specs=[vmem_spec, vmem_spec],
        out_specs=vmem_spec,
        out_shape=jax.ShapeDtypeStruct((pieces, count, columns), bf16),
        compiler_params=pltpu.CompilerParams(vmem_limit_bytes=8 * MIB),
        cost_estimate=pl.CostEstimate(
            flops=2 * count * depth * pieces * columns,
            transcendentals=0,
            bytes_accessed=2 * depth * pieces * columns,
        ),
        name="project",
    )(rows, in_vmem(weight))


def stream_kernel(rows_ref, weight_ref, after_ref, out_ref, buffer, sems):
    pieces, _, columns = out_ref.shape
    own = lax.axis_index("seq") % 2
    copies = []
    for k in range(pieces):
        first = pl.multiple_of((2 * k + own) * columns, 128)
        copies.append(
            pltpu.make_async_copy(
                weight_ref.at[:, pl.ds(first, columns)], buffer.at[k], sems.at[k]
            )
        )
    for copy in copies:
        copy.start()
    rows = rows_ref[...]
    for k in range(pieces):
        copies[k].wait()
        out_ref[k] = jnp.dot(rows, buffer[k], preferred_element_type=f32)


def project_near(rows, weight, seq_size, after):
    count, depth = rows.shape
    pieces = seq_size // 2
    columns = weight.shape[1] // seq_size
    return pl.pallas_call(
        stream_kernel,
        in_specs=[vmem_spec, any_spec, any_spec],
        out_specs=vmem_spec,
        out_shape=jax.ShapeDtypeStruct((pieces, count, columns), f32),
        scratch_shapes=[
            pltpu.VMEM((pieces, depth, columns), bf16),
            pltpu.SemaphoreType.DMA((pieces,)),
        ],
        compiler_params=pltpu.CompilerParams(vmem_limit_bytes=20 * MIB),
        cost_estimate=pl.CostEstimate(
            flops=2 * count * depth * pieces * columns,
            transcendentals=0,
            bytes_accessed=2 * depth * pieces * columns,
        ),
        name="project_near",
    )(rows, in_hbm(weight), after)


def fold_kernel(near_ref, far_ref, own_ref, *send_refs, start):
    pieces, _, columns = far_ref.shape
    here = lax.axis_index("seq") // 2
    for k in range(pieces):
        slot = (here + k) % pieces
        value = near_ref[slot, :, start : start + columns] + far_ref[slot].astype(f32)
        if k == 0:
            own_ref[...] = value
        else:
            send_refs[k - 1][...] = value.astype(bf16)


def fold(near, far, start):
    pieces, count, columns = far.shape
    return pl.pallas_call(
        functools.partial(fold_kernel, start=start),
        in_specs=[vmem_spec, vmem_spec],
        out_specs=(vmem_spec,) * pieces,
        out_shape=(jax.ShapeDtypeStruct((count, columns), f32),)
        + (jax.ShapeDtypeStruct((count, columns), bf16),) * (pieces - 1),
        compiler_params=pltpu.CompilerParams(vmem_limit_bytes=8 * MIB),
        name="fold",
    )(near, far)


def total_kernel(residual_ref, *refs):
    pieces = len(refs) // 2
    start = 0
    for group in (refs[:pieces], refs[pieces:-1]):
        if not group:
            continue
        columns = group[0].shape[1]
        value = residual_ref[:, start : start + columns].astype(f32) + group[0][...]
        for ref in group[1:]:
            value = value + ref[...].astype(f32)
        refs[-1][:, start : start + columns] = value.astype(bf16)
        start += columns


def total(residual, parts):
    operands = [residual, *parts]
    return pl.pallas_call(
        total_kernel,
        in_specs=[vmem_spec] * len(operands),
        out_specs=vmem_spec,
        out_shape=jax.ShapeDtypeStruct(residual.shape, bf16),
        compiler_params=pltpu.CompilerParams(vmem_limit_bytes=8 * MIB),
        name="total",
    )(*operands)


def vocab_kernel(*refs, shifts, base, following, first, last, halves, width_all, vocab_tile, seq_size, batch_size, drafts):
    refs = list(refs)
    blocks = len(shifts)
    row_refs = refs[: blocks * halves]
    del refs[: blocks * halves]
    gain_ref, weight_ref = refs[:2]
    del refs[:2]
    if not first:
        square_in, logit_in = refs[:2]
        del refs[:2]
    copies = []
    if last:
        ids_ref, parents_ref, out_ref, scaled_ref = refs
    elif following:
        source_ref, square_out, logit_out, next_ref, scaled_ref, sems = refs
    else:
        square_out, logit_out, scaled_ref = refs
    _, vocab, columns = weight_ref.shape
    tiles = vocab // vocab_tile
    first_of = lambda shift: pl.multiple_of(ring_slot(shift, seq_size) * columns, 128)
    firsts = [first_of(shift) for shift in shifts]
    for k, shift in enumerate(following):
        copies.append(
            pltpu.make_async_copy(
                source_ref.at[:, pl.ds(first_of(shift), columns)], next_ref.at[k], sems.at[k]
            )
        )
    for copy in copies:
        copy.start()
    square = None if first else square_in[...]
    for b in range(blocks):
        start = 0
        squares = []
        for part in range(halves):
            stream = row_refs[b * halves + part][...].astype(f32)
            rows = stream.shape[0]
            scaled_ref[b, start : start + rows, :] = (
                stream * gain_ref[:, pl.ds(firsts[b], columns)][0:1, :]
            ).astype(bf16)
            start += rows
            squared = stream * stream
            squares.append(
                sum(squared[:, k * 128 : (k + 1) * 128] for k in range(squared.shape[1] // 128))
            )
        squares = jnp.concatenate(squares, axis=0)
        square = squares if square is None else square + squares
    tokens = scaled_ref.shape[1]
    if last:
        mean = jnp.sum(jnp.transpose(square), axis=0, keepdims=True) / width_all
        shrink = lax.rsqrt(mean + norm_epsilon)
        vocab_first = (
            lax.axis_index("seq") * batch_size + lax.axis_index("batch")
        ) * vocab
        row = lax.broadcasted_iota(jnp.int32, (tokens, tokens), 0)
        choice = jnp.where(row == parents_ref[0:1, :], 1.0, 0.0).astype(bf16)
    else:
        square_out[...] = square
    tops, totals, picks = [], [], []
    for t in range(tiles):
        span = slice(t * vocab_tile, (t + 1) * vocab_tile)
        logits = None if first else logit_in[span, :]
        for b in range(blocks):
            product = lax.dot_general(
                weight_ref[base + b, span, :], scaled_ref[b], NT, preferred_element_type=f32
            )
            logits = product if logits is None else logits + product
        if not last:
            logit_out[span, :] = logits
            continue
        logits = logits * shrink
        top = jnp.max(logits, axis=0, keepdims=True)
        tops.append(top)
        totals.append(jnp.sum(jnp.exp(logits - top), axis=0, keepdims=True))
        column = lax.broadcasted_iota(jnp.int32, logits.shape, 0) + (vocab_first + t * vocab_tile)
        rest = logits
        source = None
        for _ in range(3):
            piece = rest.astype(bf16)
            rest = rest - piece.astype(f32)
            product = jnp.dot(piece, choice, preferred_element_type=f32)
            source = product if source is None else source + product
        picks.append(
            jnp.sum(jnp.where(column == ids_ref[0:1, :], source, 0.0), axis=0, keepdims=True)
        )
    for copy in copies:
        copy.wait()
    if not last:
        return
    best = functools.reduce(jnp.maximum, tops)
    mass = sum(total * jnp.exp(top - best) for top, total in zip(tops, totals))
    picked = sum(picks)
    pairs = batch_size // 2
    own = lax.axis_index("batch")
    pad = jnp.zeros((1, 128 - drafts), f32)
    for dc in range(2):
        for dx in range(pairs):
            g = (dc * pairs + dx) * drafts
            batch = ((own // 2 + dx) % pairs) * 2 + (own + dc) % 2
            line = jnp.concatenate(
                [x for v in (best, mass, picked) for x in (v[:, g : g + drafts], pad)], axis=1
            )
            for s in range(seq_size):
                out_ref[s * batch_size + batch] = line


def vocab_step(
    rows, shifts, table, base, gain, weight, sizes, drafts, state=None, final=None, following=()
):
    blocks = len(rows)
    halves = len(rows[0])
    vocab, width_all = weight.shape
    columns = rows[0][0].shape[1]
    tokens = sum(r.shape[0] for r in rows[0])
    seq_size, batch_size = sizes
    operands = [r for parts in rows for r in parts] + [gain, in_vmem(table)]
    aliases = {}
    if state is not None:
        if final is None:
            aliases = {len(operands) + k: k for k in range(2)}
        operands += list(state)
    in_specs = [vmem_spec] * len(operands)
    scratch = [pltpu.VMEM((blocks, tokens, columns), bf16)]
    if final is not None:
        operands += list(final)
        in_specs += [vmem_spec] * 2
        out_shape = jax.ShapeDtypeStruct((seq_size * batch_size, 1, 384), f32)
        out_specs = vmem_spec
    else:
        out_shape = (
            jax.ShapeDtypeStruct((tokens, 128), f32),
            jax.ShapeDtypeStruct((vocab, tokens), f32),
        )
        out_specs = (vmem_spec,) * 2
    if following:
        operands.append(in_hbm(weight))
        in_specs.append(any_spec)
        out_shape += (pltpu.VMEM((len(following), vocab, columns), bf16),)
        out_specs += (vmem_spec,)
        scratch.append(pltpu.SemaphoreType.DMA((len(following),)))
    return pl.pallas_call(
        functools.partial(
            vocab_kernel,
            shifts=tuple(shifts),
            base=base,
            following=tuple(following),
            first=state is None,
            last=final is not None,
            halves=halves,
            width_all=width_all,
            vocab_tile=min(512, vocab),
            seq_size=seq_size,
            batch_size=batch_size,
            drafts=drafts,
        ),
        in_specs=in_specs,
        out_specs=out_specs,
        out_shape=out_shape,
        scratch_shapes=scratch,
        input_output_aliases=aliases,
        compiler_params=pltpu.CompilerParams(vmem_limit_bytes=12 * MIB),
        cost_estimate=pl.CostEstimate(
            flops=2 * tokens * vocab * columns * blocks,
            transcendentals=0,
            bytes_accessed=2 * vocab * columns * blocks + 8 * vocab * tokens,
        ),
        name="vocab",
    )(*operands)


def finish_kernel(accept_ref, stats_ref, parent_ref, target_ref, accepted_ref):
    drafts = target_ref.shape[1]
    stats = stats_ref[:, 0, :]
    tops, totals, picks = (stats[:, k * 128 : (k + 1) * 128] for k in range(3))
    best = jnp.max(tops, axis=0, keepdims=True)
    mass = jnp.sum(totals * jnp.exp(tops - best), axis=0, keepdims=True)
    chosen = jnp.sum(picks, axis=0, keepdims=True)
    log_total = best + jnp.log(mass)
    column = jnp.transpose(jnp.broadcast_to(log_total, (128, 128)))[:drafts, :drafts]
    parents = parent_ref[pl.ds(lax.axis_index("batch"), 1), :]
    row = lax.broadcasted_iota(jnp.int32, (drafts, drafts), 0)
    parent_total = jnp.sum(jnp.where(row == parents, column, 0.0), axis=0, keepdims=True)
    target = chosen[:, :drafts] - parent_total
    target_ref[...] = target
    index = lax.broadcasted_iota(jnp.int32, target.shape, 1)
    accepted_ref[...] = jnp.sum(
        jnp.where(index < accept_ref[0], target, 0.0), axis=1, keepdims=True
    )


def finish(stats, parent, accept_len, drafts):
    target, accepted = pl.pallas_call(
        finish_kernel,
        in_specs=[smem_spec, vmem_spec, vmem_spec],
        out_specs=(vmem_spec, vmem_spec),
        out_shape=(jax.ShapeDtypeStruct((1, drafts), f32), jax.ShapeDtypeStruct((1, 1), f32)),
        compiler_params=pltpu.CompilerParams(vmem_limit_bytes=4 * MIB),
        name="finish",
    )(accept_len, stats, parent)
    return target, accepted.reshape(1)


def plain_tail(head_rows, residual, out_proj, norm_gain, lm_head, parent, draft_ids, accept_len):
    draft_count = head_rows.shape[0]
    batch_index = lax.axis_index("batch")
    branch_term = jnp.dot(head_rows, out_proj, preferred_element_type=f32)
    width_local = residual.shape[1]
    feature_first = lax.axis_index("seq") * width_local
    stream_mine = residual.astype(f32) + lax.psum_scatter(
        branch_term, "seq", scatter_dimension=1, tiled=True
    )
    square = lax.psum(jnp.sum(stream_mine * stream_mine, axis=1), "seq")
    width_all = width_local * lax.axis_size("seq")
    gain_mine = lax.dynamic_slice_in_dim(norm_gain, feature_first, width_local, 0)
    normed_mine = (
        stream_mine * lax.rsqrt(square / width_all + norm_epsilon)[:, None] * gain_mine
    ).astype(bf16)
    normed = lax.all_gather(normed_mine, "seq", axis=1, tiled=True)
    hidden_out = stream_mine.astype(bf16)
    vocab_rows = lm_head.shape[0]
    vocab_first = lax.axis_index(("seq", "batch")) * vocab_rows
    logits = jnp.einsum(
        "rd,vd->rv",
        lax.all_gather(normed, "batch", axis=0, tiled=True),
        lm_head,
        preferred_element_type=f32,
    )
    request_total = parent.shape[0]
    parent_rows = (
        jnp.arange(request_total, dtype=jnp.int32)[:, None] * draft_count + parent
    ).reshape(-1)
    source = logits[parent_rows]
    column = jnp.arange(vocab_rows, dtype=jnp.int32) + vocab_first
    picked = jnp.sum(
        jnp.where(column[None, :] == draft_ids.reshape(-1)[:, None], source, 0.0), axis=1
    )
    best = lax.pmax(jnp.max(logits, axis=1), ("seq", "batch"))
    exp_mass, chosen = lax.psum(
        (jnp.sum(jnp.exp(logits - best[:, None]), axis=1), picked), ("seq", "batch")
    )
    log_total = best + jnp.log(exp_mass)
    target_all = (chosen - log_total[parent_rows]).reshape(request_total, draft_count)
    target_logp = lax.dynamic_slice_in_dim(target_all, batch_index, 1, 0)
    indices = jnp.arange(draft_count, dtype=jnp.int32)
    accepted_score = jnp.sum(
        jnp.where(indices[None, :] < accept_len[:, None], target_logp, 0.0), axis=1
    )
    return (hidden_out, target_logp, accepted_score)


def body(
    q_nope,
    q_rope,
    absorb_k,
    absorb_v,
    cache_latent,
    cache_rope,
    draft_latent,
    draft_rope,
    residual,
    out_proj,
    norm_gain,
    lm_head,
    parent,
    draft_ids,
    cache_len,
    accept_len,
    *,
    seq_size,
    batch_size,
):
    requests, draft_count, local_heads, nope_width = q_nope.shape
    assert requests == 1 and seq_size % 2 == 0 and batch_size % 2 == 0
    cache_rows, width = cache_latent.shape[1:]
    rope_width = q_rope.shape[3]
    scale = math.log2(math.e) / math.sqrt(nope_width + rope_width)
    batch_index = lax.axis_index("batch")

    order = [*range(0, seq_size, 2), *reversed(range(1, seq_size, 2))]
    forward = [(order[i], order[(i + 1) % seq_size]) for i in range(seq_size)]
    backward = [(b, a) for a, b in forward]
    move = lambda array, ring: lax.ppermute(array, "seq", ring)

    units = 4
    unit = cache_rows // units
    size = unit + unit * rope_width // width
    lower, upper = pack(cache_latent[0], jnp.swapaxes(cache_rope[0], 0, 1), unit)
    far = seq_size // 2
    assert far > 1
    ahead = [move(lower, forward), move(upper, backward)]
    behind = [move(upper, forward), move(lower, backward)]

    query = jnp.einsum(
        "ihn,hnc->hic", q_nope[0], absorb_k, preferred_element_type=f32
    ).astype(bf16).reshape(local_heads * draft_count, width)
    rope = jnp.transpose(q_rope[0], (1, 0, 2)).reshape(local_heads * draft_count, rope_width)
    own_parents = lax.dynamic_slice_in_dim(parent, batch_index * requests, requests, 0)
    mask = ancestry_of(own_parents)[0]

    pairs = batch_size // 2
    own_pair, own_core = batch_index // 2, batch_index % 2
    group_batch = jnp.stack(
        [
            ((own_pair + dx) % pairs) * 2 + (own_core + dc) % 2
            for dc in range(2)
            for dx in range(pairs)
        ]
    )
    tokens = batch_size * draft_count
    id_row = draft_ids[group_batch].reshape(1, tokens)
    starts = jnp.arange(batch_size, dtype=jnp.int32)[:, None] * draft_count
    parent_row = (parent[group_batch] + starts).reshape(1, tokens)

    gain = jnp.broadcast_to(norm_gain[None, :], (8, norm_gain.shape[0]))
    run = functools.partial(
        attend,
        cache_len,
        query,
        rope,
        unit=unit,
        draft_count=draft_count,
        scale=scale,
        seq_size=seq_size,
        cache_rows=cache_rows,
    )
    state = run(
        [lower, upper], [(0, 0), (0, 2 * unit)], tree=(draft_latent[0], draft_rope[0], mask)
    )
    weight = token = late = None
    early = min(2, far - 1)
    tail = [x for k in range(early + 1, far) for x in (-k, k)] + [far]
    for k in range(1, far):
        ahead, state, token, id_row, parent_row, gain = lax.optimization_barrier(
            (ahead, state, token, id_row, parent_row, gain)
        )
        arrived = ahead
        if k < far - 1:
            ahead = [move(arrived[0], forward), move(arrived[1], backward)]
        else:
            low = [move(arrived[0][q * size : (q + 1) * size], forward) for q in range(2)]
            high = [move(arrived[1][q * size : (q + 1) * size], backward) for q in range(2)]
        state = run(arrived, [(-k, 0), (k, 2 * unit)], state=state, after=token)
        behind, state = lax.optimization_barrier((behind, state))
        arrived = behind
        if k < far - 1:
            behind = [move(arrived[0], forward), move(arrived[1], backward)]
        if k == 1 and residual.shape[1] % 128 == 0:
            weight, token = fetch(out_proj, seq_size, arrived[0])
        if k == 2 and residual.shape[1] % 128 == 0:
            late, token = fetch(lm_head, seq_size, arrived[0], shifts=tail)
        state = run(arrived, [(-k, 2 * unit), (k, 0)], state=state)
    state = run([low[0], high[0]], [(far, 0), (far, 2 * unit)], state=state, after=token)
    head_rows = run(
        [low[1], high[1]], [(far, unit), (far, 3 * unit)], state=state, absorb_v=absorb_v
    )

    columns = residual.shape[1]
    if columns % 128:
        return plain_tail(
            head_rows, residual, out_proj, norm_gain, lm_head, parent, draft_ids, accept_len
        )
    swap = [(s, s ^ 1) for s in range(seq_size)]
    split = (columns // 128 + 1) // 2 * 128
    spans = [(0, split), (split, columns - split)]
    sent = [project(head_rows, weight, *span) for span in spans]
    near = project_near(head_rows, out_proj, seq_size, sent[-1])
    sent = [lax.ppermute(x, "seq", swap) for x in sent]
    parts = []
    for (start, _), share in zip(spans, sent):
        own, *sends = fold(near, share, start)
        parts.append(own)
        for k, send in enumerate(sends):
            perm = [(s, (s + 2 * (k + 1)) % seq_size) for s in range(seq_size)]
            parts.append(lax.ppermute(send, "seq", perm))
    hidden_out = total(residual, parts)

    table, _ = fetch(lm_head, seq_size, hidden_out, shifts=(0,))
    rows = [hidden_out]
    for k in range(1, pairs):
        perm = [(((x + k) % pairs) * 2 + c, x * 2 + c) for x in range(pairs) for c in range(2)]
        rows.append(lax.ppermute(hidden_out, "batch", perm))
    rows, table = lax.optimization_barrier((rows, table))
    rows = jnp.concatenate(rows, axis=0)
    partner = [(b, b ^ 1) for b in range(batch_size)]
    twin = lambda r: (r, lax.ppermute(r, "batch", partner))
    step = functools.partial(
        vocab_step,
        gain=gain,
        weight=lm_head,
        sizes=(seq_size, batch_size),
        drafts=draft_count,
    )
    left = right = rows
    arrived = [twin(rows)]
    left = lax.ppermute(rows, "seq", forward)
    right = lax.ppermute(rows, "seq", backward)
    *state, table = step(
        arrived, (0,), table, 0, following=[x for k in range(1, early + 1) for x in (-k, k)]
    )
    left, right, state, table = lax.optimization_barrier((left, right, state, table))
    for k in range(1, far):
        arrived = [twin(left), twin(right)]
        if k < far - 1:
            left = lax.ppermute(left, "seq", forward)
            right = lax.ppermute(right, "seq", backward)
        else:
            cut = rows.shape[0] // 2
            left = lax.ppermute(left[:cut], "seq", forward)
            right = lax.ppermute(right[cut:], "seq", backward)
        source, base = (table, 2 * (k - 1)) if k <= early else (late, 2 * (k - 1 - early))
        state = step(arrived, (-k, k), source, base, state=state)
        left, right, state = lax.optimization_barrier((left, right, state))
    ends = twin(jnp.concatenate([left, right], axis=0))
    stats = step(
        [ends], (far,), late, 2 * (far - 1 - early), state=state, final=(id_row, parent_row)
    )
    stats = lax.all_to_all(stats, ("seq", "batch"), 0, 0, tiled=True)
    target_logp, accepted_score = finish(stats, parent, accept_len, draft_count)
    return (hidden_out, target_logp, accepted_score)


def solution(mesh):
    in_specs = (
        P("batch", None, "seq", None),
        P("batch", None, "seq", None),
        P("seq", None, None),
        P("seq", None, None),
        P("batch", "seq", None),
        P("batch", "seq", None),
        P("batch", None, None),
        P("batch", None, None),
        P("batch", "seq"),
        P("seq", None),
        P(),
        P(("seq", "batch"), None),
        P(),
        P(),
        P("batch"),
        P("batch"),
    )
    out_specs = (P("batch", "seq"), P("batch", None), P("batch"))
    sized = functools.partial(body, seq_size=mesh.shape["seq"], batch_size=mesh.shape["batch"])
    return jax.shard_map(sized, mesh=mesh, in_specs=in_specs, out_specs=out_specs, check_vma=False)
```
